1024 devices in a mesh: dp: 16 (over y, core), expert: 64 (over z, x).
Axes of the slice: x: 4, y: 8, z: 16, core: 2. Of those that a mesh axis runs over, the one named last changes fastest.
Arguments:
- tokens: bfloat16 [131072, 1024], P(('dp', 'expert')), may hold values from -6 to 6
- cotangent: bfloat16 [131072, 1024], P(('dp', 'expert')), may hold values from -0.1875 to 0.1875
- expert_ids: int32 [131072, 4], P(('dp', 'expert')), may hold values from 0 to 63, all different within a row; in each aligned block of 128 rows (0 to 127, 128 to 255, ...) at most 16 rows name the same one
- gate_probs: bfloat16 [131072, 4], P(('dp', 'expert')), may hold values from 0.019897461 to 0.59765625
- home_share: int32 [32], replicated, may hold values from 4 to 8
- gate_weight: bfloat16 [64, 1024, 384], P('expert'), may hold values from -0.1875 to 0.1875
- up_weight: bfloat16 [64, 1024, 384], P('expert'), may hold values from -0.1875 to 0.1875
- down_weight: bfloat16 [64, 384, 1024], P('expert'), may hold values from -0.3125 to 0.3125
Outputs:
- gate_cotangent: float32 [131072, 4], P(('dp', 'expert'))
- grad_gate: float32 [64, 1024, 384], P('expert', 'dp')
- grad_up: float32 [64, 1024, 384], P('expert', 'dp')
- grad_down: float32 [64, 384, 1024], P('expert', 'dp')
The draws below stay inside these ranges and needn't reach their ends.
Inputs may be any that keep to these rules, and one draw needn't show every extreme that they name: `expert_ids`: each token names 4 different experts; among the tokens of one device no expert is named more than 16 times.
All inputs are finite; a program needn't handle non-finite values.
Results may differ from the reference program's by a relative error of at most 0.017.
Values may be sent and summed in bfloat16 or wider, within the bound.
A program may use at most 64 MiB of HBM per device.

```python
import math
import jax
import jax.numpy as jnp
import numpy as np
from jax import lax

D = 1024
FF = 384
TOP = 4
TOK_DEV = 128
EXPERTS = 64
HALF = 32
CAP_OWN = 8
CAP_REP = 2
MOST = 16
TOKENS = 131072
N_DP = 16
N_EXPERT = 64


def place_ends(values, key, least, high):
    index_at = [jax.random.randint(jax.random.fold_in(key, axis), (), 0, length) for axis, length in enumerate(values.shape)]
    main_axis = values.shape.index(max(values.shape))
    beside = index_at[:main_axis] + [(index_at[main_axis] + 1) % values.shape[main_axis]] + index_at[main_axis + 1:]
    return values.at[tuple(index_at)].set(least).at[tuple(beside)].set(high)


def block_scale(key, dims, cuts, least, largest):
    def one(axis_at, parts):
        draws = jax.random.uniform(jax.random.fold_in(jax.random.fold_in(key, 6), axis_at), (parts,), jnp.float32, least / len(cuts), largest / len(cuts))
        return jnp.repeat(jnp.exp(draws), dims[axis_at] // parts).reshape((-1,) + (1,) * (len(dims) - axis_at - 1))

    level = one(*cuts[0])
    for cut in cuts[1:]:
        level = level * one(*cut)
    return level


def routed_block(stream_key, own, number, rows, count, top, limit, lean):
    ranking = jax.random.permutation(stream_key, count)
    crowded, usual = load_shares(count, rows * top, limit, lean, True), load_shares(count, rows * top, limit, lean, False)
    places = jnp.arange(count)

    def named(tallies, rotation):
        used = int((tallies > 0).sum())
        fixed = max(1, used // 4)
        passed = fixed + (places - fixed + rotation * (used - fixed)) % max(1, count - fixed)
        return jnp.zeros((count,), jnp.int32).at[ranking[jnp.where(places < fixed, places, passed)]].set(jnp.asarray(tallies, jnp.int32))

    tallies = jnp.where(number % 4 == 0, named(crowded, number // 4), named(usual, number - number // 4 - 1))
    mixed = jax.random.permutation(jax.random.fold_in(own, 3), count)
    source_of, sink = mixed[0:count // 2 * 2:2], mixed[1:count // 2 * 2:2]
    margin = jnp.minimum(tallies[source_of] - 1, limit - tallies[sink]) // 2
    margin = jnp.where((source_of == ranking[0]) | (sink == ranking[0]) | (tallies[sink] == 0), 0, jnp.maximum(margin, 0))
    passed = jax.random.randint(jax.random.fold_in(own, 4), (count // 2,), 0, 1 << 20) % (margin + 1)
    tallies = tallies.at[source_of].add(-passed).at[sink].add(passed)
    labels = jnp.searchsorted(jnp.cumsum(tallies), jnp.arange(rows * top), side="right").astype(jnp.int32)
    grid = labels.reshape(top, rows).T
    grid = grid[jax.random.permutation(jax.random.fold_in(own, 1), rows)]
    rotation = jax.random.randint(jax.random.fold_in(own, 2), (rows, 1), 0, top)
    return jnp.take_along_axis(grid, (jnp.arange(top)[None, :] + rotation) % top, axis=1)


def load_shares(count, total, reach, lean, full):
    weights = [(1 << 20) // math.isqrt(grade ** lean) + 1 for grade in range(1, count + 1)]
    largest = reach if full else min(reach, max(-(-total // count), total * weights[0] // sum(weights)))
    least = 1 if total - largest >= count - 1 else 0
    given, spare = [largest] + [least] * (count - 1), total - largest - least * (count - 1)
    while spare > 0:
        movable = [i for i in range(1, count) if given[i] < largest] or [i for i in range(1, count) if given[i] < reach]
        mass, budget = sum([weights[i] for i in movable]), spare
        for i in movable:
            extra = min(reach - given[i], max(1, budget * weights[i] // mass), spare)
            given[i] = given[i] + extra
            spare = spare - extra
    return np.array(given)


def scatter_about(own_key, dims, scale, bound, shards=(), held_as=jnp.bfloat16):
    drawn = scale * jax.random.normal(own_key, dims, jnp.float32)
    if shards:
        drawn = drawn * block_scale(own_key, dims, shards, -0.22, 0.18)
    return jnp.clip(drawn, -bound, bound).astype(held_as)


def setup_inputs(seed: int = 0) -> dict:
    keys = jax.random.split(jax.random.key(seed), 9)
    tokens = scatter_about(keys[0], (TOKENS, D), 1.0, 6.0, ((0, 1024),))
    cotangent = scatter_about(keys[1], (TOKENS, D), 0.03125, 0.1875, ((0, 1024),))
    expert_ids_keys = jax.random.split(jax.random.fold_in(keys[2], 1), TOKENS // TOK_DEV)
    expert_ids_turns = jax.random.permutation(jax.random.fold_in(keys[2], 3), TOKENS // TOK_DEV)
    expert_ids = jax.vmap(lambda own, number: routed_block(jax.random.fold_in(keys[2], 2), own, number, TOK_DEV, EXPERTS, TOP, MOST, 2))(expert_ids_keys, expert_ids_turns).reshape((TOKENS, TOP))
    gate_probs = jnp.clip(jnp.exp(math.log(0.59765625) - 3.4024236 * jax.random.uniform(keys[3], (TOKENS, TOP), jnp.float32) ** block_scale(keys[3], (TOKENS, TOP), ((0, 1024),), -0.2, 0.2)), 0.019897461, 0.59765625).astype(jnp.bfloat16)
    home_share = place_ends(jax.random.randint(keys[4], (HALF,), CAP_OWN // 2, CAP_OWN + 1), jax.random.fold_in(keys[4], 1), CAP_OWN // 2, CAP_OWN).astype(jnp.int32)
    gate_weight = scatter_about(keys[5], (EXPERTS, D, FF), D ** -0.5, 0.1875, ((0, 64),))
    up_weight = scatter_about(keys[6], (EXPERTS, D, FF), D ** -0.5, 0.1875, ((0, 64),))
    down_weight = scatter_about(keys[7], (EXPERTS, FF, D), FF ** -0.5, 0.3125, ((0, 64),))
    return {"tokens": tokens, "cotangent": cotangent, "expert_ids": expert_ids, "gate_probs": gate_probs, "home_share": home_share, "gate_weight": gate_weight, "up_weight": up_weight, "down_weight": down_weight}


def route_rows(expert_ids, home_share, experts, cap_own, cap_rep):
    half_axis = experts // 2
    capacity = cap_own + cap_rep
    flat_ids = expert_ids.reshape(-1).astype(jnp.int32)
    columns = jnp.arange(experts, dtype=jnp.int32)
    onehot = (flat_ids[:, None] == columns[None, :]).astype(jnp.int32)
    before = jnp.cumsum(onehot, axis=0) - onehot
    row_rank = jnp.sum(before * onehot, axis=1)
    limits = jnp.concatenate([home_share.astype(jnp.int32), jnp.full((experts - half_axis,), cap_own, jnp.int32)])
    home_limit = jnp.sum(onehot * limits[None, :], axis=1)
    at_home = row_rank < home_limit
    overflow = row_rank - home_limit
    to_copy = (flat_ids < half_axis) & (overflow >= 0) & (overflow < cap_rep)
    target = jnp.where(to_copy, flat_ids + half_axis, flat_ids)
    slot_index = jnp.where(to_copy, cap_own + overflow, row_rank)
    position = jnp.where(at_home | to_copy, target * capacity + slot_index, experts * capacity)
    return position.reshape(expert_ids.shape).astype(jnp.int32)


def dot_exact(left, right):
    return jnp.dot(left.astype(jnp.float32), right.astype(jnp.float32), precision=lax.Precision.HIGHEST)


def expert_side(inputs, grads_out, weights_row, gate_weight, up_weight, down_weight):
    gate_act = dot_exact(inputs, gate_weight)
    up_act = dot_exact(inputs, up_weight)
    sigmoid_gate = jax.nn.sigmoid(gate_act)
    silu_gate = gate_act * sigmoid_gate
    hidden = (silu_gate * up_act).astype(jnp.bfloat16)
    output = dot_exact(hidden, down_weight)
    upstream = grads_out.astype(jnp.float32)
    gate_cot = jnp.sum(upstream * output, axis=1)
    scaled = (weights_row.astype(jnp.float32)[:, None] * upstream).astype(jnp.bfloat16)
    hidden_cot = dot_exact(scaled, down_weight.T)
    gate_pre = (hidden_cot * up_act * sigmoid_gate * (1.0 + gate_act * (1.0 - sigmoid_gate))).astype(jnp.bfloat16)
    up_pre = (hidden_cot * silu_gate).astype(jnp.bfloat16)
    grad_gate = dot_exact(inputs.T, gate_pre)
    grad_up = dot_exact(inputs.T, up_pre)
    grad_down = dot_exact(hidden.T, scaled)
    return gate_cot, grad_gate, grad_up, grad_down


def reference(tokens, cotangent, expert_ids, gate_probs, home_share, gate_weight, up_weight, down_weight):
    experts = EXPERTS
    half_axis = experts // 2
    capacity = CAP_OWN + CAP_REP
    slots_total = N_EXPERT * capacity
    model_width = D

    def pack(tok_block, cot_block, prob_block, position):
        spread = position.shape + (model_width,)
        row_buffer = jnp.zeros((slots_total + 1, model_width), tok_block.dtype)
        row_buffer = row_buffer.at[position].set(jnp.broadcast_to(tok_block[:, None, :], spread))
        cot_buffer = jnp.zeros((slots_total + 1, model_width), cot_block.dtype)
        cot_buffer = cot_buffer.at[position].set(jnp.broadcast_to(cot_block[:, None, :], spread))
        prob_buffer = jnp.zeros((slots_total + 1,), prob_block.dtype).at[position].set(prob_block)
        return row_buffer[:-1], cot_buffer[:-1], prob_buffer[:-1]

    def group_step(totals, group):
        tok_group, cot_group, id_group, prob_group = group
        positions = jax.vmap(lambda blocks: route_rows(blocks, home_share, experts, CAP_OWN, CAP_REP))(id_group)
        send_rows, send_cots, send_probs = jax.vmap(pack)(tok_group, cot_group, prob_group, positions)
        recv_rows = jnp.swapaxes(send_rows.reshape(N_EXPERT, N_EXPERT, capacity, model_width), 0, 1)
        recv_cots = jnp.swapaxes(send_cots.reshape(N_EXPERT, N_EXPERT, capacity, model_width), 0, 1)
        recv_probs = jnp.swapaxes(send_probs.reshape(N_EXPERT, N_EXPERT, capacity), 0, 1)

        def device_step(device):
            slot_rows = recv_rows[device]
            slot_cots = recv_cots[device]
            slot_probs = recv_probs[device]
            home_part = expert_side(slot_rows[:, :CAP_OWN].reshape(-1, model_width), slot_cots[:, :CAP_OWN].reshape(-1, model_width), slot_probs[:, :CAP_OWN].reshape(-1), gate_weight[device], up_weight[device], down_weight[device])
            source = (device - half_axis) % experts
            copy_part = expert_side(slot_rows[:, CAP_OWN:].reshape(-1, model_width), slot_cots[:, CAP_OWN:].reshape(-1, model_width), slot_probs[:, CAP_OWN:].reshape(-1), gate_weight[source], up_weight[source], down_weight[source])
            gate_cot = jnp.concatenate([home_part[0].reshape(N_EXPERT, CAP_OWN), copy_part[0].reshape(N_EXPERT, CAP_REP)], axis=1)
            return gate_cot, home_part[1:], copy_part[1:]

        gate_cot, home_grads, copy_grads = lax.map(device_step, jnp.arange(experts, dtype=jnp.int32))
        returned = jnp.swapaxes(gate_cot, 0, 1).reshape(N_EXPERT, slots_total)

        def unpack(back_row, position):
            return jnp.concatenate([back_row, jnp.zeros((1,), jnp.float32)])[position]

        group_cot = jax.vmap(unpack)(returned, positions)
        new_totals = []
        for total, home_grad, copy_grad in zip(totals, home_grads, copy_grads):
            copy_bf = lax.optimization_barrier(copy_grad.astype(jnp.bfloat16)).astype(jnp.float32)
            home_bf = lax.optimization_barrier(home_grad.astype(jnp.bfloat16)).astype(jnp.float32)
            at_home = jnp.concatenate([copy_bf[half_axis:], jnp.zeros_like(copy_bf[:experts - half_axis])])
            new_totals.append(total + home_bf + at_home)
        return tuple(new_totals), group_cot

    def shaped(array):
        return array.reshape((N_DP, N_EXPERT, TOK_DEV) + array.shape[1:])

    start = (jnp.zeros((experts, D, FF), jnp.float32), jnp.zeros((experts, D, FF), jnp.float32), jnp.zeros((experts, FF, D), jnp.float32))
    totals, group_cots = lax.scan(group_step, start, (shaped(tokens), shaped(cotangent), shaped(expert_ids), shaped(gate_probs)))
    return group_cots.reshape(TOKENS, TOP), totals[0], totals[1], totals[2]
```

```python
import functools

import jax
import jax.numpy as jnp
from jax import lax
from jax.experimental import pallas as pl
from jax.experimental.pallas import tpu as pltpu
from jax.sharding import PartitionSpec as P

MESH = pl.DeviceIdType.MESH
CAP_OWN = 8
CAP_REP = 2
NX = 4
DROPPED = 99.0
F32 = jnp.float32
BF16 = jnp.bfloat16
VMEM = pl.BlockSpec(memory_space=pltpu.VMEM)
ANY = pl.BlockSpec(memory_space=pl.ANY)


def dot(a, b, dims=((1,), (0,))):
    return lax.dot_general(a, b, (dims, ((), ())), preferred_element_type=F32)


def pack_kernel(ids_ref, prob_ref, cap_ref, tok_ref, cot_ref, base_ref, ext_ref, rank_ref, pw_ref):
    experts, toks = rank_ref.shape
    half, _, wide = ext_ref.shape
    row = lax.broadcasted_iota(jnp.int32, (experts, toks), 0)
    named = jnp.zeros((experts, toks), F32)
    weight = jnp.zeros((experts, toks), F32)
    for k in range(ids_ref.shape[0]):
        hit = ids_ref[k : k + 1, :] == row
        named += jnp.where(hit, 1.0, 0.0)
        weight += jnp.where(hit, prob_ref[k : k + 1, :], 0.0)
    earlier = lax.broadcasted_iota(jnp.int32, (toks, toks), 0) < lax.broadcasted_iota(jnp.int32, (toks, toks), 1)
    before = dot(named.astype(BF16), jnp.where(earlier, 1.0, 0.0).astype(BF16))
    kept = (named > 0.5) & (before < cap_ref[...])
    rank_ref[...] = jnp.where(kept, before, DROPPED)
    pw_ref[...] = weight

    group = 8

    @pl.loop(0, experts // group)
    def _(b):
        at = pl.ds(pl.multiple_of(b * group, group), group)
        shape = (group, 16, toks)
        slot = lax.broadcasted_iota(jnp.int32, shape, 1).astype(F32)
        ranks = jnp.broadcast_to(rank_ref[at, :].reshape(group, 1, toks), shape)
        weights = jnp.broadcast_to(pw_ref[at, :].reshape(group, 1, toks), shape)
        pick = jnp.where((ranks == slot) & (slot < 7.5), 1.0, 0.0).reshape(group * 16, toks).astype(BF16)
        scale = jnp.where(ranks == slot - 8.0, weights, 0.0).reshape(group * 16, toks).astype(BF16)
        rows = dot(pick, tok_ref[...]) + dot(scale, cot_ref[...])
        base_ref[at] = rows.reshape(group, 16, rows.shape[1]).astype(BF16)

    big = 16 if half % 16 == 0 else half

    @pl.loop(0, half // big)
    def _(b):
        at = pl.ds(pl.multiple_of(b * big, big), big)
        shape = (big, 8, toks)
        place = lax.broadcasted_iota(jnp.int32, shape, 1)
        ranks = jnp.broadcast_to(rank_ref[at, :].reshape(big, 1, toks), shape)
        weights = jnp.broadcast_to(pw_ref[at, :].reshape(big, 1, toks), shape)
        here = ranks == (8 + place % 2).astype(F32)
        total = jnp.zeros((big * 8, wide), F32)
        for q in range(2):
            pick = jnp.where(here & (place // 2 == 2 * q), 1.0, 0.0).reshape(big * 8, toks).astype(BF16)
            scale = jnp.where(here & (place // 2 == 2 * q + 1), weights, 0.0).reshape(big * 8, toks).astype(BF16)
            cols = slice(q * wide, (q + 1) * wide)
            total += dot(pick, tok_ref[:, cols]) + dot(scale, cot_ref[:, cols])
        ext_ref[at] = total.reshape(big, 8, wide).astype(BF16)


def partner(k, nz, zx):
    z, x = zx
    j = k // NX
    odd = j % 2
    dz = nz // 2 + (1 - odd) * (j // 2) - odd * ((j + 1) // 2)
    pz = lax.rem(z + dz + nz, nz)
    px = lax.rem(x + lax.rem(k, NX) + 1, NX)
    return pz, px


def send_kernel(nz, base_ref, ext_ref, rb_ref, re_ref, bsend, brecv, esend, erecv, lsem):
    me = lax.axis_index("expert")
    zx = (me // NX, lax.rem(me, NX))
    experts = nz * NX
    half = experts // 2
    low = me < half
    barrier = pltpu.get_barrier_semaphore()

    def greet(k, c):
        pz, px = partner(k, nz, zx)
        pl.semaphore_signal(barrier, inc=1, device_id={"expert": pz * NX + px}, device_id_type=MESH)
        return c

    lax.fori_loop(0, experts - 1, greet, 0)
    own = pltpu.make_async_copy(base_ref.at[me], rb_ref.at[me], lsem.at[0])
    own.start()
    pl.semaphore_wait(barrier, experts - 1)

    def base_copy(k, peer):
        return pltpu.make_async_remote_copy(
            src_ref=base_ref.at[peer],
            dst_ref=rb_ref.at[me],
            send_sem=bsend.at[k],
            recv_sem=brecv.at[k],
            device_id={"expert": peer},
            device_id_type=MESH,
        )

    def ext_copy(k, peer):
        return pltpu.make_async_remote_copy(
            src_ref=ext_ref.at[peer],
            dst_ref=re_ref.at[me],
            send_sem=esend.at[k],
            recv_sem=erecv.at[k],
            device_id={"expert": peer},
            device_id_type=MESH,
        )

    def issue(k, c):
        pz, px = partner(k, nz, zx)
        peer = pz * NX + px
        base_copy(k, peer).start()

        @pl.when(peer < half)
        def _():
            ext_copy(k, peer).start()

        return c

    lax.fori_loop(0, experts - 1, issue, 0)

    @pl.when(low)
    def _():
        mine = pltpu.make_async_copy(ext_ref.at[me], re_ref.at[me], lsem.at[1])
        mine.start()
        mine.wait()

    def finish(k, c):
        pz, px = partner(k, nz, zx)
        peer = pz * NX + px
        base_copy(k, peer).wait()

        @pl.when(peer < half)
        def _():
            ext_copy(k, peer).wait_send()

        @pl.when(low)
        def _():
            ext_copy(k, 0).wait_recv()

        return c

    lax.fori_loop(0, experts - 1, finish, 0)
    own.wait()


def expert_kernel(
    flag_ref, rb_ref, re_ref, wg_ref, wu_ref, wd_ref,
    gate_ref, up_ref, dl_ref, dr_ref, v_ref,
    x_ref, s_ref, h_ref, pg_ref, pu_ref, ve_ref,
):
    sources, _, d = rb_ref.shape
    wide = d // 2
    ff = wg_ref.shape[1]
    base = sources * 8
    block = 128
    low = flag_ref[0] > 0

    @pl.loop(0, base // block)
    def _(b):
        part = rb_ref[pl.ds(b * (block // 8), block // 8)].astype(F32)
        at = pl.ds(pl.multiple_of(b * block, block), block)
        x_ref[at, :] = part[:, :8, :].reshape(block, d).astype(BF16)
        s_ref[at, :] = part[:, 8:, :].reshape(block, d).astype(BF16)

    extra = re_ref[...].astype(F32).reshape(sources * 8, wide)
    extra = jnp.where(low, extra, 0.0).astype(BF16)
    out_row = lax.broadcasted_iota(jnp.int32, (4 * sources, sources * 8), 0)
    in_row = lax.broadcasted_iota(jnp.int32, (4 * sources, sources * 8), 1)
    wanted = (out_row % sources) * 8 + out_row // sources
    for q in range(2):
        pick = jnp.where(in_row == wanted + 4 * q, 1.0, 0.0).astype(BF16)
        rows = dot(pick, extra).astype(BF16)
        cols = slice(q * wide, (q + 1) * wide)
        x_ref[base : base + 2 * sources, cols] = rows[: 2 * sources]
        s_ref[base : base + 2 * sources, cols] = rows[2 * sources :]

    def side(at, rows):
        x, s = x_ref[at, :], s_ref[at, :]
        a = dot(x, wg_ref[...])
        b = dot(x, wu_ref[...])
        sig = jax.nn.sigmoid(a)
        silu = a * sig
        hidden = (silu * b).astype(BF16)
        h_ref[at, :] = hidden
        cot = dot(s, wd_ref[...], ((1,), (1,)))
        pg_ref[at, :] = (cot * b * sig * (1.0 + a * (1.0 - sig))).astype(BF16)
        pu_ref[at, :] = (cot * silu).astype(BF16)
        out = dot(hidden, wd_ref[...])
        return jnp.sum(out * s.astype(F32), axis=1, keepdims=True)

    col = side(pl.ds(base, 2 * sources), 2 * sources)
    lane = lax.broadcasted_iota(jnp.int32, (sources, 128), 1)
    ve_ref[...] = jnp.where(lane == 8, col[:sources], 0.0) + jnp.where(lane == 9, col[sources:], 0.0)

    @pl.loop(0, base // block)
    def _(b):
        at = pl.ds(pl.multiple_of(b * block, block), block)
        col = side(at, block)
        few = block // 8
        shape = (block, 128)
        lane = lax.broadcasted_iota(jnp.int32, shape, 1)
        sub = lax.broadcasted_iota(jnp.int32, shape, 0) % 8
        tile = jnp.where(lane == sub, col, 0.0).reshape(few, 8, 128)
        src = pl.ds(pl.multiple_of(b * few, few), few)
        extra = jnp.broadcast_to(ve_ref[src, :].reshape(few, 1, 128), (few, 8, 128))
        first = lax.broadcasted_iota(jnp.int32, (few, 8, 128), 1) == 0
        v_ref[src] = tile + jnp.where(first, extra, 0.0)

    ny, _, share, _ = gate_ref.shape
    turn = (((0,), (0,)))
    for y in range(ny):
        xs = x_ref[:, y * 2 * share : (y + 1) * 2 * share]
        gate_ref[y] = dot(xs, pg_ref[...], turn).reshape(2, share, ff).astype(BF16)
        up_ref[y] = dot(xs, pu_ref[...], turn).reshape(2, share, ff).astype(BF16)
    few = dl_ref.shape[2]
    pair = ny * 2 * few
    step = min(128, pair)
    for side_ref, at in ((dl_ref, 0), (dr_ref, wide)):
        down = dot(h_ref[...], s_ref[:, at : at + wide], turn)
        side_ref[...] = down.reshape(ny, 2, few, wide).astype(BF16)


def ring_kernel(
    nz, ids_ref, prob_ref, rank_ref, v_ref, gate_ref, up_ref, dl_ref, dr_ref,
    gc_out, gate_out, up_out, down_out,
    vr_ref, peer_g, peer_u, peer_l, peer_r,
    out_g, out_u, out_l, out_r, in_g, in_u, in_l, in_r,
    vsend, vrecv, dsend, drecv, rsend, rrecv,
):
    me = lax.axis_index("expert")
    zx = (me // NX, lax.rem(me, NX))
    experts = nz * NX
    dp = lax.axis_index("dp")
    y, core = dp // 2, lax.rem(dp, 2)
    ny = gate_ref.shape[0]
    barrier = pltpu.get_barrier_semaphore()
    other = 1 - core
    ahead = lax.rem(y + 1, ny) * 2 + core
    behind = lax.rem(y + ny - 1, ny) * 2 + core

    def greet(k, c):
        pz, px = partner(k, nz, zx)
        pl.semaphore_signal(barrier, inc=1, device_id={"expert": pz * NX + px}, device_id_type=MESH)
        return c

    for near in (y * 2 + other, ahead, behind):
        pl.semaphore_signal(barrier, inc=1, device_id={"dp": near}, device_id_type=MESH)
    lax.fori_loop(0, experts - 1, greet, 0)
    pl.semaphore_wait(barrier, experts - 1 + 3)

    parts = (
        (gate_ref, peer_g, out_g, in_g, 1),
        (up_ref, peer_u, out_u, in_u, -1),
        (dl_ref, peer_l, out_l, in_l, 1),
        (dr_ref, peer_r, out_r, in_r, -1),
    )

    def owner(way, s):
        return lax.rem(y - way * (1 + s) + 2 * ny, ny)

    def across(i, s):
        src, dst, _, _, way = parts[i]
        o = owner(way, s)
        return pltpu.make_async_remote_copy(
            src_ref=src.at[o, other],
            dst_ref=dst.at[o],
            send_sem=dsend.at[i, s],
            recv_sem=drecv.at[i, s],
            device_id={"dp": y * 2 + other},
            device_id_type=MESH,
        )

    for s in range(ny):
        for i in range(4):
            across(i, s).start()

    def v_copy(k):
        pz, px = partner(k, nz, zx)
        peer = pz * NX + px
        return pltpu.make_async_remote_copy(
            src_ref=v_ref.at[peer],
            dst_ref=vr_ref.at[me],
            send_sem=vsend.at[k],
            recv_sem=vrecv.at[k],
            device_id={"expert": peer},
            device_id_type=MESH,
        )

    def v_issue(k, c):
        v_copy(k).start()
        return c

    lax.fori_loop(0, experts - 1, v_issue, 0)
    vr_ref[pl.ds(me, 1)] = v_ref[pl.ds(me, 1)]

    def hop(i, s):
        _, _, out, inn, way = parts[i]
        return pltpu.make_async_remote_copy(
            src_ref=out.at[s],
            dst_ref=inn.at[s],
            send_sem=rsend.at[i, s],
            recv_sem=rrecv.at[i, s],
            device_id={"dp": ahead if way == 1 else behind},
            device_id_type=MESH,
        )

    def local(i, s):
        src, dst, _, _, way = parts[i]
        o = owner(way, s)
        across(i, s).wait()
        return src[o, core].astype(F32) + dst[o].astype(F32)

    for s in range(ny - 1):
        for i in range(4):
            _, _, out, inn, _ = parts[i]
            total = local(i, s)
            if s > 0:
                hop(i, s - 1).wait_recv()
                total = total + inn[s - 1].astype(F32)
            out[s] = total.astype(BF16)
            hop(i, s).start()
    wide = dl_ref.shape[3]
    for i, ref in ((0, gate_out), (1, up_out), (2, down_out), (3, down_out)):
        total = local(i, ny - 1)
        hop(i, ny - 2).wait_recv()
        total = total + parts[i][3][ny - 2].astype(F32)
        if i < 2:
            ref[...] = total
        else:
            ref[:, (i - 2) * wide : (i - 1) * wide] = total
    for s in range(ny - 1):
        for i in range(4):
            hop(i, s).wait_send()

    def v_finish(k, c):
        v_copy(k).wait()
        return c

    lax.fori_loop(0, experts - 1, v_finish, 0)
    values = jnp.sum(vr_ref[...], axis=1)
    rank = rank_ref[...]
    back = jnp.zeros(rank.shape, F32)
    for r in range(CAP_OWN + CAP_REP):
        back += jnp.where(rank == float(r), values[:, r : r + 1], 0.0)
    row = lax.broadcasted_iota(jnp.int32, rank.shape, 0)
    for k in range(ids_ref.shape[0]):
        mine = jnp.where(ids_ref[k : k + 1, :] == row, back, 0.0)
        gc_out[k : k + 1, :] = jnp.sum(mine, axis=0, keepdims=True) / prob_ref[k : k + 1, :]


def per_device(tokens, cotangent, expert_ids, gate_probs, home_share, gate_weight, up_weight, down_weight):
    experts = lax.axis_size("expert")
    groups = lax.axis_size("dp")
    nz, ny = experts // NX, groups // 2
    half = experts // 2
    toks, d = tokens.shape
    top = expert_ids.shape[1]
    ff = gate_weight.shape[2]
    wide = d // 2
    share, few = d // groups, ff // groups
    shape = jax.ShapeDtypeStruct

    ids = expert_ids.T
    probs = gate_probs.T.astype(F32)
    cap = jnp.concatenate([home_share + CAP_REP, jnp.full((experts - half,), CAP_OWN, jnp.int32)]).astype(F32)[:, None]
    base, ext, rank = pl.pallas_call(
        pack_kernel,
        out_shape=(shape((experts, 16, d), BF16), shape((half, 8, wide), BF16), shape((experts, toks), F32)),
        in_specs=[VMEM] * 5,
        out_specs=(VMEM,) * 3,
        scratch_shapes=[pltpu.VMEM((experts, toks), F32)],
        name="pack",
    )(ids, probs, cap, tokens, cotangent)

    dma = pltpu.SemaphoreType.DMA
    rb, re = pl.pallas_call(
        functools.partial(send_kernel, nz),
        out_shape=(shape((experts, 16, d), BF16), shape((experts, 8, wide), BF16)),
        in_specs=[ANY] * 2,
        out_specs=(ANY,) * 2,
        scratch_shapes=[dma((experts,)), dma((experts,)), dma((experts,)), dma((experts,)), dma((2,))],
        compiler_params=pltpu.CompilerParams(collective_id=0, has_side_effects=True),
        name="dispatch",
    )(base, ext)

    flag = (lax.axis_index("expert") < half).astype(jnp.int32).reshape(1)
    rows = experts * 10
    gate, up, dl, dr, v = pl.pallas_call(
        expert_kernel,
        out_shape=(
            shape((ny, 2, share, ff), BF16),
            shape((ny, 2, share, ff), BF16),
            shape((ny, 2, few, wide), BF16),
            shape((ny, 2, few, wide), BF16),
            shape((experts, 8, 128), F32),
        ),
        in_specs=[pl.BlockSpec(memory_space=pltpu.SMEM)] + [VMEM] * 5,
        out_specs=(VMEM,) * 5,
        scratch_shapes=[
            pltpu.VMEM((rows, d), BF16),
            pltpu.VMEM((rows, d), BF16),
            pltpu.VMEM((rows, ff), BF16),
            pltpu.VMEM((rows, ff), BF16),
            pltpu.VMEM((rows, ff), BF16),
            pltpu.VMEM((experts, 128), F32),
        ],
        name="expert",
    )(flag, rb, re, gate_weight[0], up_weight[0], down_weight[0])

    gu = (share, ff)
    dn = (few, wide)
    gc, gg, gup, gdn = pl.pallas_call(
        functools.partial(ring_kernel, nz),
        out_shape=(shape((top, toks), F32), shape(gu, F32), shape(gu, F32), shape((few, d), F32)),
        in_specs=[VMEM] * 8,
        out_specs=(VMEM,) * 4,
        scratch_shapes=[pltpu.VMEM((experts, 8, 128), F32)]
        + [pltpu.VMEM((ny,) + s, BF16) for s in (gu, gu, dn, dn)]
        + [pltpu.VMEM((ny - 1,) + s, BF16) for s in (gu, gu, dn, dn)] * 2
        + [dma((experts,)), dma((experts,)), dma((4, ny)), dma((4, ny)), dma((4, ny)), dma((4, ny))],
        compiler_params=pltpu.CompilerParams(collective_id=1, has_side_effects=True),
        name="reduce",
    )(ids, probs, rank, v, gate, up, dl, dr)
    return gc.T, gg[None], gup[None], gdn[None]


def solution(mesh):
    rows = P(("dp", "expert"), None)
    held = P("expert", None, None)
    split = P("expert", "dp", None)
    return jax.shard_map(
        per_device,
        mesh=mesh,
        in_specs=(rows, rows, rows, rows, P(), held, held, held),
        out_specs=(rows, split, split, split),
        check_vma=False,
    )
```

```python
import functools

import jax
import jax.numpy as jnp
from jax import lax
from jax.experimental import pallas as pl
from jax.experimental.pallas import tpu as pltpu
from jax.sharding import PartitionSpec as P

MESH = pl.DeviceIdType.MESH
CAP_OWN = 8
CAP_REP = 2
NX = 4
DROPPED = 99.0
F32 = jnp.float32
BF16 = jnp.bfloat16
VMEM = pl.BlockSpec(memory_space=pltpu.VMEM)
ANY = pl.BlockSpec(memory_space=pl.ANY)


def dot(a, b, dims=((1,), (0,))):
    return lax.dot_general(a, b, (dims, ((), ())), preferred_element_type=F32)


def partner(k, nz, zx):
    z, x = zx
    j = k // NX
    odd = j % 2
    dz = nz // 2 + (1 - odd) * (j // 2) - odd * ((j + 1) // 2)
    pz = lax.rem(z + dz + nz, nz)
    px = lax.rem(x + lax.rem(k, NX) + 1, NX)
    return pz, px


def origin(k, nz, zx):
    z, x = zx
    j = k // NX
    odd = j % 2
    dz = nz // 2 + (1 - odd) * (j // 2) - odd * ((j + 1) // 2)
    oz = lax.rem(z - dz + 2 * nz, nz)
    ox = lax.rem(x - lax.rem(k, NX) - 1 + 2 * NX, NX)
    return oz, ox


def layer_kernel(
    nz, ids_ref, prob_ref, home_ref, tok_ref, cot_ref, wg_hbm, wu_hbm, wd_hbm,
    gc_out, gate_out, up_out, down_out,
    rank_ref, pw_ref, base_ref, ext_ref, rb_ref, re_ref,
    wg_ref, wu_ref, wd_ref, x_ref, s_ref, h_ref, pg_ref, pu_ref, v_ref, vr_ref,
    gate_ref, up_ref, dl_ref, dr_ref, peer_g, peer_u, peer_l, peer_r,
    out_g, out_u, out_l, out_r, in_g, in_u, in_l, in_r,
    wsem, bsend, brecv, esend, erecv, vsend, vrecv, dsend, drecv, rsend, rrecv,
):
    me = lax.axis_index("expert")
    zx = (me // NX, lax.rem(me, NX))
    experts = nz * NX
    half = experts // 2
    last = experts - 1
    low = me < half
    dp = lax.axis_index("dp")
    y, core = dp // 2, lax.rem(dp, 2)
    ny = gate_ref.shape[0]
    other = 1 - core
    ahead = lax.rem(y + 1, ny) * 2 + core
    behind = lax.rem(y + ny - 1, ny) * 2 + core
    toks, d = tok_ref.shape
    top = ids_ref.shape[1]
    ff = wg_ref.shape[1]
    wide = d // 2
    barrier = pltpu.get_barrier_semaphore()

    def at_partner(k):
        pz, px = partner(k, nz, zx)
        return pz * NX + px

    def greet(k, c):
        pl.semaphore_signal(barrier, inc=1, device_id={"expert": at_partner(k)}, device_id_type=MESH)
        return c

    lax.fori_loop(0, last, greet, 0)
    for near in (y * 2 + other, ahead, behind):
        pl.semaphore_signal(barrier, inc=1, device_id={"dp": near}, device_id_type=MESH)
    loads = [
        pltpu.make_async_copy(src, dst, wsem.at[i])
        for i, (src, dst) in enumerate(((wg_hbm, wg_ref), (wu_hbm, wu_ref), (wd_hbm, wd_ref)))
    ]
    for load in loads:
        load.start()

    lane = lax.broadcasted_iota(jnp.int32, (toks, experts), 1)
    named = jnp.zeros((toks, experts), F32)
    weight = jnp.zeros((toks, experts), F32)
    for k in range(top):
        hit = ids_ref[:, k : k + 1] == lane
        named += jnp.where(hit, 1.0, 0.0)
        weight += jnp.where(hit, prob_ref[:, k : k + 1].astype(F32), 0.0)
    named, weight = named.astype(BF16), weight.astype(BF16)
    first = lax.broadcasted_iota(jnp.int32, (toks, toks), 0)
    second = lax.broadcasted_iota(jnp.int32, (toks, toks), 1)
    unit = jnp.where(first == second, 1.0, 0.0).astype(BF16)
    earlier = jnp.where(first < second, 1.0, 0.0).astype(BF16)
    turn = ((0,), (0,))
    home = home_ref[...].astype(F32) + CAP_REP
    home_lane = lax.broadcasted_iota(jnp.int32, (experts, half), 1)
    home_row = lax.broadcasted_iota(jnp.int32, (experts, half), 0)
    cap = jnp.sum(jnp.where(home_lane == home_row, home, 0.0), axis=1, keepdims=True)
    cap = jnp.where(lax.broadcasted_iota(jnp.int32, (experts, 1), 0) < half, cap, float(CAP_OWN))
    before = dot(named, earlier, turn)
    kept = (dot(named, unit, turn) > 0.5) & (before < cap)
    rank_ref[...] = jnp.where(kept, before, DROPPED)
    pw_ref[...] = dot(weight, unit, turn)

    group = 8

    @pl.loop(0, experts // group)
    def _(b):
        at = pl.ds(pl.multiple_of(b * group, group), group)
        shape = (group, 16, toks)
        slot = lax.broadcasted_iota(jnp.int32, shape, 1).astype(F32)
        ranks = jnp.broadcast_to(rank_ref[at, :].reshape(group, 1, toks), shape)
        weights = jnp.broadcast_to(pw_ref[at, :].reshape(group, 1, toks), shape)
        pick = jnp.where((ranks == slot) & (slot < 7.5), 1.0, 0.0).reshape(group * 16, toks).astype(BF16)
        scale = jnp.where(ranks == slot - 8.0, weights, 0.0).reshape(group * 16, toks).astype(BF16)
        rows = dot(pick, tok_ref[...]) + dot(scale, cot_ref[...])
        base_ref[at] = rows.reshape(group, 16, d).astype(BF16)

    big = 16 if half % 16 == 0 else half

    @pl.loop(0, half // big)
    def _(b):
        at = pl.ds(pl.multiple_of(b * big, big), big)
        shape = (big, 8, toks)
        place = lax.broadcasted_iota(jnp.int32, shape, 1)
        ranks = jnp.broadcast_to(rank_ref[at, :].reshape(big, 1, toks), shape)
        weights = jnp.broadcast_to(pw_ref[at, :].reshape(big, 1, toks), shape)
        here = ranks == (8 + place % 2).astype(F32)
        total = jnp.zeros((big * 8, wide), F32)
        for q in range(2):
            pick = jnp.where(here & (place // 2 == 2 * q), 1.0, 0.0).reshape(big * 8, toks).astype(BF16)
            scale = jnp.where(here & (place // 2 == 2 * q + 1), weights, 0.0).reshape(big * 8, toks).astype(BF16)
            cols = slice(q * wide, (q + 1) * wide)
            total += dot(pick, tok_ref[:, cols]) + dot(scale, cot_ref[:, cols])
        ext_ref[at] = total.reshape(big, 8, wide).astype(BF16)

    pl.semaphore_wait(barrier, last + 3)

    def base_copy(k, peer):
        return pltpu.make_async_remote_copy(
            src_ref=base_ref.at[peer],
            dst_ref=rb_ref.at[k],
            send_sem=bsend.at[k],
            recv_sem=brecv.at[k],
            device_id={"expert": peer},
            device_id_type=MESH,
        )

    def ext_copy(k, peer):
        return pltpu.make_async_remote_copy(
            src_ref=ext_ref.at[peer],
            dst_ref=re_ref.at[k],
            send_sem=esend.at[k],
            recv_sem=erecv.at[k],
            device_id={"expert": peer},
            device_id_type=MESH,
        )

    def issue(k, c):
        peer = at_partner(k)
        base_copy(k, peer).start()

        @pl.when(peer < half)
        def _():
            ext_copy(k, peer).start()

        return c

    lax.fori_loop(0, last, issue, 0)
    rb_ref[last] = base_ref[me]

    @pl.when(low)
    def _():
        re_ref[last] = ext_ref[me]

    for load in loads:
        load.wait()

    many = 16
    rows = many * 10

    def v_copy(k):
        oz, ox = origin(k, nz, zx)
        return pltpu.make_async_remote_copy(
            src_ref=v_ref.at[k],
            dst_ref=vr_ref.at[me],
            send_sem=vsend.at[k],
            recv_sem=vrecv.at[k],
            device_id={"expert": oz * NX + ox},
            device_id_type=MESH,
        )

    def v_issue(k, c):
        v_copy(k).start()
        return c

    def on_group(g, c):
        def arrive(i, c2):
            k = g * many + i

            @pl.when(k < last)
            def _():
                base_copy(k, me).wait_recv()

            @pl.when((k < last) & low)
            def _():
                ext_copy(k, 0).wait_recv()

            return c2

        lax.fori_loop(0, many, arrive, 0)
        src = pl.ds(pl.multiple_of(g * many, many), many)
        at = pl.multiple_of(g * rows, 32)
        part = rb_ref[src].astype(F32)
        x_ref[pl.ds(at, many * 8), :] = part[:, :8, :].reshape(many * 8, d).astype(BF16)
        s_ref[pl.ds(at, many * 8), :] = part[:, 8:, :].reshape(many * 8, d).astype(BF16)
        extra = re_ref[src].astype(F32).reshape(many * 8, wide)
        extra = jnp.where(low, extra, 0.0).astype(BF16)
        out_row = lax.broadcasted_iota(jnp.int32, (4 * many, many * 8), 0)
        in_row = lax.broadcasted_iota(jnp.int32, (4 * many, many * 8), 1)
        wanted = (out_row % many) * 8 + out_row // many
        for q in range(2):
            pick = jnp.where(in_row == wanted + 4 * q, 1.0, 0.0).astype(BF16)
            both = dot(pick, extra).astype(BF16)
            cols = slice(q * wide, (q + 1) * wide)
            x_ref[pl.ds(at + many * 8, many * 2), cols] = both[: 2 * many]
            s_ref[pl.ds(at + many * 8, many * 2), cols] = both[2 * many :]
        here = pl.ds(at, rows)
        x, s = x_ref[here, :], s_ref[here, :]
        a = dot(x, wg_ref[...])
        b = dot(x, wu_ref[...])
        sig = jax.nn.sigmoid(a)
        silu = a * sig
        hidden = (silu * b).astype(BF16)
        h_ref[here, :] = hidden
        cot = dot(s, wd_ref[...], ((1,), (1,)))
        pg_ref[here, :] = (cot * b * sig * (1.0 + a * (1.0 - sig))).astype(BF16)
        pu_ref[here, :] = (cot * silu).astype(BF16)
        out = dot(hidden, wd_ref[...])
        col = jnp.sum(out * s.astype(F32), axis=1, keepdims=True)
        own = lax.broadcasted_iota(jnp.int32, (many * 8, 128), 1)
        sub = lax.broadcasted_iota(jnp.int32, (many * 8, 128), 0) % 8
        tile = jnp.sum(jnp.where(own == sub, col[: many * 8], 0.0).reshape(many, 8, 128), axis=1)
        own = lax.broadcasted_iota(jnp.int32, (many, 128), 1)
        for j in range(2):
            tile += jnp.where(own == 8 + j, col[many * (8 + j) : many * (9 + j)], 0.0)
        v_ref[src] = tile.reshape(many, 1, 128)
        return c

    groups = experts // many

    def do_group(g, c):
        on_group(g, c)
        lax.fori_loop(g * many, g * many + many, v_issue, 0)
        return c

    lax.fori_loop(0, groups - 1, do_group, 0)
    on_group(groups - 1, 0)

    parts = (
        (gate_ref, peer_g, out_g, in_g, 1),
        (up_ref, peer_u, out_u, in_u, -1),
        (dl_ref, peer_l, out_l, in_l, 1),
        (dr_ref, peer_r, out_r, in_r, -1),
    )

    def owner(way, s):
        return lax.rem(y - way * (1 + s) + 2 * ny, ny)

    def across(i, s):
        src, dst, _, _, way = parts[i]
        o = owner(way, s)
        return pltpu.make_async_remote_copy(
            src_ref=src.at[o, other],
            dst_ref=dst.at[o],
            send_sem=dsend.at[i, s],
            recv_sem=drecv.at[i, s],
            device_id={"dp": y * 2 + other},
            device_id_type=MESH,
        )

    def hop(i, s):
        _, _, out, inn, way = parts[i]
        return pltpu.make_async_remote_copy(
            src_ref=out.at[s],
            dst_ref=inn.at[s],
            send_sem=rsend.at[i, s],
            recv_sem=rrecv.at[i, s],
            device_id={"dp": ahead if way == 1 else behind},
            device_id_type=MESH,
        )

    share, few = gate_ref.shape[2], dl_ref.shape[2]

    def product(i, s):
        ref, way, pre = ((gate_ref, 1, pg_ref), (up_ref, -1, pu_ref))[i]
        o = owner(way, s)
        xs = x_ref[:, pl.ds(pl.multiple_of(o * 2 * share, 2 * share), 2 * share)]
        ref[o] = dot(xs, pre[...], turn).reshape(2, share, ff).astype(BF16)

    def local(i, s):
        src, dst, _, _, way = parts[i]
        o = owner(way, s)
        across(i, s).wait()
        return src[o, core].astype(F32) + dst[o].astype(F32)

    def ring(s):
        for i in range(4):
            _, _, out, inn, _ = parts[i]
            total = local(i, s)
            if s > 0:
                hop(i, s - 1).wait_recv()
                total = total + inn[s - 1].astype(F32)
            out[s] = total.astype(BF16)
            hop(i, s).start()

    product(0, 0)
    product(1, 0)
    for ref, at in ((dl_ref, 0), (dr_ref, wide)):
        down = dot(h_ref[...], s_ref[:, at : at + wide], turn)
        ref[...] = down.reshape(ny, 2, few, wide).astype(BF16)
    for i in range(2):
        across(i, 0).start()
    for s in range(ny):
        for i in range(2, 4):
            across(i, s).start()
    lax.fori_loop(last - many + 1, last, v_issue, 0)
    vr_ref[me] = v_ref[last]
    for s in range(1, ny):
        product(0, s)
        product(1, s)
        for i in range(2):
            across(i, s).start()
        if s >= 2:
            ring(s - 2)
    ring(ny - 2)

    def v_finish(k, c):
        v_copy(k).wait()
        return c

    lax.fori_loop(0, last, v_finish, 0)
    values = jnp.transpose(vr_ref[...].reshape(experts, 128))
    place = dot(jnp.where(second < first, 1.0, 0.0).astype(BF16), named)
    back = jnp.zeros((toks, experts), F32)
    for r in range(CAP_OWN + CAP_REP):
        back += jnp.where(place == float(r), values[r : r + 1, :], 0.0)
    home = jnp.concatenate([home, jnp.full((1, experts - half), float(CAP_OWN), F32)], axis=1)
    back = jnp.where(place < home, back, 0.0)
    for k in range(top):
        mine = jnp.where(ids_ref[:, k : k + 1] == lane, back, 0.0)
        gc_out[:, k : k + 1] = jnp.sum(mine, axis=1, keepdims=True) / prob_ref[:, k : k + 1].astype(F32)

    for i, ref in ((0, gate_out), (1, up_out), (2, down_out), (3, down_out)):
        total = local(i, ny - 1)
        hop(i, ny - 2).wait_recv()
        total = total + parts[i][3][ny - 2].astype(F32)
        if i < 2:
            ref[...] = total
        else:
            ref[:, (i - 2) * wide : (i - 1) * wide] = total
    for s in range(ny - 1):
        for i in range(4):
            hop(i, s).wait_send()

    def sent(k, c):
        base_copy(k, me).wait_send()

        @pl.when(at_partner(k) < half)
        def _():
            ext_copy(k, 0).wait_send()

        return c

    lax.fori_loop(0, last, sent, 0)


def pass_kernel(*refs):
    n = len(refs) // 2
    for src, dst in zip(refs[:n], refs[n:]):
        dst[...] = src[...]


def per_device(tokens, cotangent, expert_ids, gate_probs, home_share, gate_weight, up_weight, down_weight):
    experts = lax.axis_size("expert")
    groups = lax.axis_size("dp")
    nz, ny = experts // NX, groups // 2
    half = experts // 2
    toks, d = tokens.shape
    top = expert_ids.shape[1]
    ff = gate_weight.shape[2]
    wide = d // 2
    share, few = d // groups, ff // groups
    shape = jax.ShapeDtypeStruct
    dma = pltpu.SemaphoreType.DMA
    rows = experts * 10
    gu = (share, ff)
    dn = (few, wide)
    outs = (shape((toks, top), F32), shape(gu, F32), shape(gu, F32), shape((few, d), F32))

    def held(*dims, dtype=BF16):
        return pltpu.VMEM(dims, dtype)

    raw = pl.pallas_call(
        functools.partial(layer_kernel, nz),
        out_shape=outs,
        in_specs=[VMEM] * 5 + [ANY] * 3,
        out_specs=(VMEM,) * 4,
        scratch_shapes=[
            held(experts, toks, dtype=F32),
            held(experts, toks, dtype=F32),
            held(experts, 16, d),
            held(half, 8, wide),
            held(experts, 16, d),
            held(experts, 8, wide),
            held(d, ff),
            held(d, ff),
            held(ff, d),
            held(rows, d),
            held(rows, d),
            held(rows, ff),
            held(rows, ff),
            held(rows, ff),
            held(experts, 1, 128, dtype=F32),
            held(experts, 1, 128, dtype=F32),
        ]
        + [held(ny, 2, *s) for s in (gu, gu, dn, dn)]
        + [held(ny, *s) for s in (gu, gu, dn, dn)]
        + [held(ny - 1, *s) for s in (gu, gu, dn, dn)] * 2
        + [dma((3,))]
        + [dma((experts,))] * 6
        + [dma((4, ny))] * 4,
        compiler_params=pltpu.CompilerParams(collective_id=0, has_side_effects=True),
        name="layer",
    )(expert_ids, gate_probs, home_share[None], tokens, cotangent, gate_weight[0], up_weight[0], down_weight[0])
    gc, gg, gup, gdn = pl.pallas_call(
        pass_kernel, out_shape=outs, in_specs=[VMEM] * 4, out_specs=(VMEM,) * 4, name="hand_on"
    )(*raw)
    return gc, gg[None], gup[None], gdn[None]


def solution(mesh):
    rows = P(("dp", "expert"), None)
    held = P("expert", None, None)
    split = P("expert", "dp", None)
    return jax.shard_map(
        per_device,
        mesh=mesh,
        in_specs=(rows, rows, rows, rows, P(), held, held, held),
        out_specs=(rows, split, split, split),
        check_vma=False,
    )
```

```python
import functools

import jax
import jax.numpy as jnp
from jax import lax
from jax.experimental import pallas as pl
from jax.experimental.pallas import tpu as pltpu
from jax.sharding import PartitionSpec as P

MESH = pl.DeviceIdType.MESH
CAP_OWN = 8
CAP_REP = 2
NX = 4
DROPPED = 99.0
F32 = jnp.float32
BF16 = jnp.bfloat16
VMEM = pl.BlockSpec(memory_space=pltpu.VMEM)
ANY = pl.BlockSpec(memory_space=pl.ANY)


def dot(a, b, dims=((1,), (0,))):
    return lax.dot_general(a, b, (dims, ((), ())), preferred_element_type=F32)


def partner(k, nz, zx):
    z, x = zx
    j = k // NX
    odd = j % 2
    dz = nz // 2 + (1 - odd) * (j // 2) - odd * ((j + 1) // 2)
    pz = lax.rem(z + dz + nz, nz)
    px = lax.rem(x + lax.rem(k, NX) + 1, NX)
    return pz, px


def origin(k, nz, zx):
    z, x = zx
    j = k // NX
    odd = j % 2
    dz = nz // 2 + (1 - odd) * (j // 2) - odd * ((j + 1) // 2)
    oz = lax.rem(z - dz + 2 * nz, nz)
    ox = lax.rem(x - lax.rem(k, NX) - 1 + 2 * NX, NX)
    return oz, ox


def layer_kernel(
    nz, ids_ref, prob_ref, home_ref, tok_ref, cot_ref, wg_hbm, wu_hbm, wd_hbm,
    gc_out, gate_out, up_out, down_out,
    rank_ref, pw_ref, base_ref, ext_ref, rb_ref, re_ref,
    wg_ref, wu_ref, wd_ref, x_ref, s_ref, h_ref, pg_ref, pu_ref, v_ref, vr_ref,
    gate_ref, up_ref, dl_ref, dr_ref, peer_g, peer_u, peer_l, peer_r,
    out_g, out_u, out_l, out_r, in_g, in_u, in_l, in_r,
    wsem, bsend, brecv, esend, erecv, vsend, vrecv, dsend, drecv, rsend, rrecv,
):
    me = lax.axis_index("expert")
    zx = (me // NX, lax.rem(me, NX))
    experts = nz * NX
    half = experts // 2
    last = experts - 1
    low = me < half
    dp = lax.axis_index("dp")
    y, core = dp // 2, lax.rem(dp, 2)
    ny = gate_ref.shape[0]
    other = 1 - core
    ahead = lax.rem(y + 1, ny) * 2 + core
    behind = lax.rem(y + ny - 1, ny) * 2 + core
    toks, d = tok_ref.shape
    top = ids_ref.shape[0]
    ff = wg_ref.shape[1]
    wide = d // 2
    barrier = pltpu.get_barrier_semaphore()

    def at_partner(k):
        pz, px = partner(k, nz, zx)
        return pz * NX + px

    def greet(k, c):
        pl.semaphore_signal(barrier, inc=1, device_id={"expert": at_partner(k)}, device_id_type=MESH)
        return c

    lax.fori_loop(0, last, greet, 0)
    for near in (y * 2 + other, ahead, behind):
        pl.semaphore_signal(barrier, inc=1, device_id={"dp": near}, device_id_type=MESH)
    loads = [
        pltpu.make_async_copy(src, dst, wsem.at[i])
        for i, (src, dst) in enumerate(((wg_hbm, wg_ref), (wu_hbm, wu_ref), (wd_hbm, wd_ref)))
    ]
    for load in loads:
        load.start()

    turn = ((0,), (0,))
    row = lax.broadcasted_iota(jnp.int32, (experts, toks), 0)
    probs = prob_ref[...].astype(F32)
    named = jnp.zeros((experts, toks), F32)
    weight = jnp.zeros((experts, toks), F32)
    for k in range(top):
        hit = ids_ref[k : k + 1, :] == row
        named += jnp.where(hit, 1.0, 0.0)
        weight += jnp.where(hit, probs[k : k + 1, :], 0.0)
    first = lax.broadcasted_iota(jnp.int32, (toks, toks), 0)
    second = lax.broadcasted_iota(jnp.int32, (toks, toks), 1)
    earlier = jnp.where(first < second, 1.0, 0.0).astype(BF16)
    home = home_ref[...].astype(F32) + CAP_REP
    home_lane = lax.broadcasted_iota(jnp.int32, (experts, half), 1)
    home_row = lax.broadcasted_iota(jnp.int32, (experts, half), 0)
    cap = jnp.sum(jnp.where(home_lane == home_row, home, 0.0), axis=1, keepdims=True)
    cap = jnp.where(lax.broadcasted_iota(jnp.int32, (experts, 1), 0) < half, cap, float(CAP_OWN))
    before = dot(named.astype(BF16), earlier)
    kept = (named > 0.5) & (before < cap)
    rank_ref[...] = jnp.where(kept, before, DROPPED)
    pw_ref[...] = weight

    group = 8

    @pl.loop(0, experts // group)
    def _(b):
        at = pl.ds(pl.multiple_of(b * group, group), group)
        shape = (group, 16, toks)
        slot = lax.broadcasted_iota(jnp.int32, shape, 1).astype(F32)
        ranks = jnp.broadcast_to(rank_ref[at, :].reshape(group, 1, toks), shape)
        weights = jnp.broadcast_to(pw_ref[at, :].reshape(group, 1, toks), shape)
        pick = jnp.where((ranks == slot) & (slot < 7.5), 1.0, 0.0).reshape(group * 16, toks).astype(BF16)
        scale = jnp.where(ranks == slot - 8.0, weights, 0.0).reshape(group * 16, toks).astype(BF16)
        rows = dot(pick, tok_ref[...]) + dot(scale, cot_ref[...])
        base_ref[at] = rows.reshape(group, 16, d).astype(BF16)

    big = 16 if half % 16 == 0 else half

    @pl.loop(0, half // big)
    def _(b):
        at = pl.ds(pl.multiple_of(b * big, big), big)
        shape = (big, 8, toks)
        place = lax.broadcasted_iota(jnp.int32, shape, 1)
        ranks = jnp.broadcast_to(rank_ref[at, :].reshape(big, 1, toks), shape)
        weights = jnp.broadcast_to(pw_ref[at, :].reshape(big, 1, toks), shape)
        here = ranks == (8 + place % 2).astype(F32)
        total = jnp.zeros((big * 8, wide), F32)
        for q in range(2):
            pick = jnp.where(here & (place // 2 == 2 * q), 1.0, 0.0).reshape(big * 8, toks).astype(BF16)
            scale = jnp.where(here & (place // 2 == 2 * q + 1), weights, 0.0).reshape(big * 8, toks).astype(BF16)
            cols = slice(q * wide, (q + 1) * wide)
            total += dot(pick, tok_ref[:, cols]) + dot(scale, cot_ref[:, cols])
        ext_ref[at] = total.reshape(big, 8, wide).astype(BF16)

    pl.semaphore_wait(barrier, last + 3)

    def base_copy(k, peer):
        return pltpu.make_async_remote_copy(
            src_ref=base_ref.at[peer],
            dst_ref=rb_ref.at[k],
            send_sem=bsend.at[k],
            recv_sem=brecv.at[k],
            device_id={"expert": peer},
            device_id_type=MESH,
        )

    def ext_copy(k, peer):
        return pltpu.make_async_remote_copy(
            src_ref=ext_ref.at[peer],
            dst_ref=re_ref.at[k],
            send_sem=esend.at[k],
            recv_sem=erecv.at[k],
            device_id={"expert": peer},
            device_id_type=MESH,
        )

    def issue(k, c):
        peer = at_partner(k)
        base_copy(k, peer).start()

        @pl.when(peer < half)
        def _():
            ext_copy(k, peer).start()

        return c

    lax.fori_loop(0, last, issue, 0)
    rb_ref[last] = base_ref[me]

    @pl.when(low)
    def _():
        re_ref[last] = ext_ref[me]

    for load in loads:
        load.wait()

    many = 16
    rows = many * 10

    def v_copy(k):
        oz, ox = origin(k, nz, zx)
        return pltpu.make_async_remote_copy(
            src_ref=v_ref.at[k],
            dst_ref=vr_ref.at[me],
            send_sem=vsend.at[k],
            recv_sem=vrecv.at[k],
            device_id={"expert": oz * NX + ox},
            device_id_type=MESH,
        )

    def v_issue(k, c):
        v_copy(k).start()
        return c

    def on_group(g, c):
        def arrive(i, c2):
            k = g * many + i

            @pl.when(k < last)
            def _():
                base_copy(k, me).wait_recv()

            @pl.when((k < last) & low)
            def _():
                ext_copy(k, 0).wait_recv()

            return c2

        lax.fori_loop(0, many, arrive, 0)
        src = pl.ds(pl.multiple_of(g * many, many), many)
        at = pl.multiple_of(g * rows, 32)
        part = rb_ref[src].astype(F32)
        x_ref[pl.ds(at, many * 8), :] = part[:, :8, :].reshape(many * 8, d).astype(BF16)
        s_ref[pl.ds(at, many * 8), :] = part[:, 8:, :].reshape(many * 8, d).astype(BF16)
        extra = re_ref[src].astype(F32).reshape(many * 8, wide)
        extra = jnp.where(low, extra, 0.0).astype(BF16)
        out_row = lax.broadcasted_iota(jnp.int32, (4 * many, many * 8), 0)
        in_row = lax.broadcasted_iota(jnp.int32, (4 * many, many * 8), 1)
        wanted = (out_row % many) * 8 + out_row // many
        for q in range(2):
            pick = jnp.where(in_row == wanted + 4 * q, 1.0, 0.0).astype(BF16)
            both = dot(pick, extra).astype(BF16)
            cols = slice(q * wide, (q + 1) * wide)
            x_ref[pl.ds(at + many * 8, many * 2), cols] = both[: 2 * many]
            s_ref[pl.ds(at + many * 8, many * 2), cols] = both[2 * many :]
        here = pl.ds(at, rows)
        x, s = x_ref[here, :], s_ref[here, :]
        a = dot(x, wg_ref[...])
        b = dot(x, wu_ref[...])
        sig = jax.nn.sigmoid(a)
        silu = a * sig
        hidden = (silu * b).astype(BF16)
        h_ref[here, :] = hidden
        cot = dot(s, wd_ref[...], ((1,), (1,)))
        pg_ref[here, :] = (cot * b * sig * (1.0 + a * (1.0 - sig))).astype(BF16)
        pu_ref[here, :] = (cot * silu).astype(BF16)
        out = dot(hidden, wd_ref[...])
        col = jnp.sum(out * s.astype(F32), axis=1, keepdims=True)
        own = lax.broadcasted_iota(jnp.int32, (many * 8, 128), 1)
        sub = lax.broadcasted_iota(jnp.int32, (many * 8, 128), 0) % 8
        tile = jnp.sum(jnp.where(own == sub, col[: many * 8], 0.0).reshape(many, 8, 128), axis=1)
        own = lax.broadcasted_iota(jnp.int32, (many, 128), 1)
        for j in range(2):
            tile += jnp.where(own == 8 + j, col[many * (8 + j) : many * (9 + j)], 0.0)
        v_ref[src] = tile.reshape(many, 1, 128)
        return c

    groups = experts // many

    def do_group(g, c):
        on_group(g, c)
        lax.fori_loop(g * many, g * many + many, v_issue, 0)
        return c

    lax.fori_loop(0, groups - 1, do_group, 0)
    on_group(groups - 1, 0)

    far = ny // 2
    parts = (
        (gate_ref, peer_g, out_g, in_g),
        (up_ref, peer_u, out_u, in_u),
        (dl_ref, peer_l, out_l, in_l),
        (dr_ref, peer_r, out_r, in_r),
    )
    ways = (1, -1)

    def length(i, w):
        return far if (i % 2 == 0) == (w == 0) else ny - 1 - far

    def chip(off):
        return lax.rem(y + off + ny, ny)

    def across(i, off):
        src, dst, _, _ = parts[i]
        o = chip(off)
        return pltpu.make_async_remote_copy(
            src_ref=src.at[o, other],
            dst_ref=dst.at[o],
            send_sem=dsend.at[i, off % ny],
            recv_sem=drecv.at[i, off % ny],
            device_id={"dp": y * 2 + other},
            device_id_type=MESH,
        )

    def hop(i, w, t):
        _, _, out, inn = parts[i]
        at = w * far + t
        return pltpu.make_async_remote_copy(
            src_ref=out.at[at],
            dst_ref=inn.at[at],
            send_sem=rsend.at[i, at],
            recv_sem=rrecv.at[i, at],
            device_id={"dp": ahead if w == 0 else behind},
            device_id_type=MESH,
        )

    share, few = gate_ref.shape[2], dl_ref.shape[2]

    def product(off):
        o = chip(off)
        xs = x_ref[:, pl.ds(pl.multiple_of(o * 2 * share, 2 * share), 2 * share)]
        gate_ref[o] = dot(xs, pg_ref[...], turn).reshape(2, share, ff).astype(BF16)
        up_ref[o] = dot(xs, pu_ref[...], turn).reshape(2, share, ff).astype(BF16)

    def cross(off, which):
        for i in which:
            across(i, off).start()

    joined = set()

    def local(i, off):
        if (i, off % ny) not in joined:
            joined.add((i, off % ny))
            across(i, off).wait()
        src, dst, _, _ = parts[i]
        o = chip(off)
        return src[o, core].astype(F32) + dst[o].astype(F32)

    def ring(t):
        chains = [(i, w) for i in range(4) for w in range(2)]
        chains.sort(key=lambda c: -length(*c))
        for i, w in chains:
            if t < length(i, w):
                total = local(i, ways[w] * (length(i, w) - t))
                if t > 0:
                    hop(i, w, t - 1).wait_recv()
                    total = total + parts[i][3][w * far + t - 1].astype(F32)
                parts[i][2][w * far + t] = total.astype(BF16)
                hop(i, w, t).start()

    steps = [far]
    for m in range(far - 1, 0, -1):
        steps += [m, -m]
    steps += [0]
    product(far)
    for ref, at in ((dl_ref, 0), (dr_ref, wide)):
        down = dot(h_ref[...], s_ref[:, at : at + wide], turn)
        ref[...] = down.reshape(ny, 2, few, wide).astype(BF16)
    cross(far, range(4))
    lax.fori_loop(last - many + 1, last, v_issue, 0)
    vr_ref[me] = v_ref[last]
    t = 0
    for n, off in enumerate(steps[1:]):
        product(off)
        cross(off, range(4))
        if n % 2 == 1:
            ring(t)
            t += 1
    for rest in range(t, far):
        ring(rest)

    def v_finish(k, c):
        v_copy(k).wait()
        return c

    lax.fori_loop(0, last, v_finish, 0)
    values = vr_ref[...].reshape(experts, 128)
    place = rank_ref[...]
    back = jnp.zeros((experts, toks), F32)
    for r in range(CAP_OWN + CAP_REP):
        back += jnp.where(place == float(r), values[:, r : r + 1], 0.0)
    for k in range(top):
        mine = jnp.where(ids_ref[k : k + 1, :] == row, back, 0.0)
        gc_out[k : k + 1, :] = jnp.sum(mine, axis=0, keepdims=True) / probs[k : k + 1, :]

    for i, ref in ((0, gate_out), (1, up_out), (2, down_out), (3, down_out)):
        total = local(i, 0)
        for w in range(2):
            if length(i, w) > 0:
                hop(i, w, length(i, w) - 1).wait_recv()
                total = total + parts[i][3][w * far + length(i, w) - 1].astype(F32)
        if i < 2:
            ref[...] = total
        else:
            ref[:, (i - 2) * wide : (i - 1) * wide] = total
    for i in range(4):
        for w in range(2):
            for t in range(length(i, w)):
                hop(i, w, t).wait_send()

    def sent(k, c):
        base_copy(k, me).wait_send()

        @pl.when(at_partner(k) < half)
        def _():
            ext_copy(k, 0).wait_send()

        return c

    lax.fori_loop(0, last, sent, 0)


def pass_kernel(*refs):
    n = len(refs) // 2
    for src, dst in zip(refs[:n], refs[n:]):
        dst[...] = src[...]


def per_device(tokens, cotangent, expert_ids, gate_probs, home_share, gate_weight, up_weight, down_weight):
    experts = lax.axis_size("expert")
    groups = lax.axis_size("dp")
    nz, ny = experts // NX, groups // 2
    half = experts // 2
    toks, d = tokens.shape
    top = expert_ids.shape[1]
    ff = gate_weight.shape[2]
    wide = d // 2
    share, few = d // groups, ff // groups
    shape = jax.ShapeDtypeStruct
    dma = pltpu.SemaphoreType.DMA
    rows = experts * 10
    gu = (share, ff)
    dn = (few, wide)
    outs = (shape((top, toks), F32), shape(gu, F32), shape(gu, F32), shape((few, d), F32))

    def held(*dims, dtype=BF16):
        return pltpu.VMEM(dims, dtype)

    raw = pl.pallas_call(
        functools.partial(layer_kernel, nz),
        out_shape=outs,
        in_specs=[VMEM] * 5 + [ANY] * 3,
        out_specs=(VMEM,) * 4,
        scratch_shapes=[
            held(experts, toks, dtype=F32),
            held(experts, toks, dtype=F32),
            held(experts, 16, d),
            held(half, 8, wide),
            held(experts, 16, d),
            held(experts, 8, wide),
            held(d, ff),
            held(d, ff),
            held(ff, d),
            held(rows, d),
            held(rows, d),
            held(rows, ff),
            held(rows, ff),
            held(rows, ff),
            held(experts, 1, 128, dtype=F32),
            held(experts, 1, 128, dtype=F32),
        ]
        + [held(ny, 2, *s) for s in (gu, gu, dn, dn)]
        + [held(ny, *s) for s in (gu, gu, dn, dn)]
        + [held(ny, *s) for s in (gu, gu, dn, dn)] * 2
        + [dma((3,))]
        + [dma((experts,))] * 6
        + [dma((4, ny))] * 4,
        compiler_params=pltpu.CompilerParams(collective_id=0, has_side_effects=True),
        name="layer",
    )(expert_ids.T, gate_probs.T, home_share[None], tokens, cotangent, gate_weight[0], up_weight[0], down_weight[0])
    gc, gg, gup, gdn = pl.pallas_call(
        pass_kernel, out_shape=outs, in_specs=[VMEM] * 4, out_specs=(VMEM,) * 4, name="hand_on"
    )(*raw)
    return gc.T, gg[None], gup[None], gdn[None]


def solution(mesh):
    rows = P(("dp", "expert"), None)
    held = P("expert", None, None)
    split = P("expert", "dp", None)
    return jax.shard_map(
        per_device,
        mesh=mesh,
        in_specs=(rows, rows, rows, rows, P(), held, held, held),
        out_specs=(rows, split, split, split),
        check_vma=False,
    )
```

```python
import functools

import jax
import jax.numpy as jnp
from jax import lax
from jax.experimental import pallas as pl
from jax.experimental.pallas import tpu as pltpu
from jax.sharding import PartitionSpec as P

MESH = pl.DeviceIdType.MESH
CAP_OWN = 8
CAP_REP = 2
NX = 4
DROPPED = 99.0
F32 = jnp.float32
BF16 = jnp.bfloat16
VMEM = pl.BlockSpec(memory_space=pltpu.VMEM)
ANY = pl.BlockSpec(memory_space=pl.ANY)


def dot(a, b, dims=((1,), (0,))):
    return lax.dot_general(a, b, (dims, ((), ())), preferred_element_type=F32)


def partner(k, nz, zx):
    z, x = zx
    j = k // NX
    odd = j % 2
    dz = nz // 2 + (1 - odd) * (j // 2) - odd * ((j + 1) // 2)
    pz = lax.rem(z + dz + nz, nz)
    px = lax.rem(x + lax.rem(k, NX) + 1, NX)
    return pz, px


def toward(b):
    odd = b % 2
    return odd * ((b + 1) // 2) - (1 - odd) * (b // 2)


def origin(k, nz, zx):
    z, x = zx
    oz = lax.rem(z - toward(k // NX) + 2 * nz, nz)
    ox = lax.rem(x - lax.rem(k, NX) + NX, NX)
    return oz, ox


def layer_kernel(
    nz, ids_ref, prob_ref, home_ref, tok_ref, cot_ref, wg_hbm, wu_hbm, wd_hbm,
    gc_out, gate_out, up_out, down_out,
    rank_ref, seen_ref, seen_pw_ref, meta_ref, blk_ref, base_ref, ext_ref, rb_ref, re_ref,
    wg_ref, wu_ref, wd_ref, x_ref, s_ref, h_ref, pg_ref, pu_ref, v_ref, vr_ref,
    gate_ref, up_ref, dl_ref, dr_ref, peer_g, peer_u, peer_l, peer_r,
    out_g, out_u, out_l, out_r, in_g, in_u, in_l, in_r,
    wsem, bsend, brecv, esend, erecv, vsend, vrecv, msend, mrecv, gsend, grecv, dsend, drecv, rsend, rrecv,
):
    me = lax.axis_index("expert")
    zx = (me // NX, lax.rem(me, NX))
    experts = nz * NX
    half = experts // 2
    last = experts - 1
    low = me < half
    dp = lax.axis_index("dp")
    y, core = dp // 2, lax.rem(dp, 2)
    ny = gate_ref.shape[0]
    other = 1 - core
    ahead = lax.rem(y + 1, ny) * 2 + core
    behind = lax.rem(y + ny - 1, ny) * 2 + core
    toks, d = tok_ref.shape
    top = ids_ref.shape[0]
    ff = wg_ref.shape[1]
    wide = d // 2
    barrier = pltpu.get_barrier_semaphore()

    def at_partner(k):
        pz, px = partner(k, nz, zx)
        return pz * NX + px

    def greet(k, c):
        pl.semaphore_signal(barrier, inc=1, device_id={"expert": at_partner(k)}, device_id_type=MESH)
        return c

    lax.fori_loop(0, last, greet, 0)
    for near in (y * 2 + other, ahead, behind):
        pl.semaphore_signal(barrier, inc=1, device_id={"dp": near}, device_id_type=MESH)
    loads = [
        pltpu.make_async_copy(src, dst, wsem.at[i])
        for i, (src, dst) in enumerate(((wg_hbm, wg_ref), (wu_hbm, wu_ref), (wd_hbm, wd_ref)))
    ]
    for load in loads:
        load.start()

    turn = ((0,), (0,))
    row = lax.broadcasted_iota(jnp.int32, (experts, toks), 0)
    probs = prob_ref[...].astype(F32)
    named = jnp.zeros((experts, toks), F32)
    for k in range(top):
        named += jnp.where(ids_ref[k : k + 1, :] == row, 1.0, 0.0)
    meta_ref[0] = jnp.concatenate([ids_ref[...].astype(F32), probs], axis=0)
    first = lax.broadcasted_iota(jnp.int32, (toks, toks), 0)
    second = lax.broadcasted_iota(jnp.int32, (toks, toks), 1)
    earlier = jnp.where(first < second, 1.0, 0.0).astype(BF16)
    home = home_ref[...].astype(F32) + CAP_REP
    home_lane = lax.broadcasted_iota(jnp.int32, (experts, half), 1)
    home_row = lax.broadcasted_iota(jnp.int32, (experts, half), 0)
    cap = jnp.sum(jnp.where(home_lane == home_row, home, 0.0), axis=1, keepdims=True)
    cap = jnp.where(lax.broadcasted_iota(jnp.int32, (experts, 1), 0) < half, cap, float(CAP_OWN))
    before = dot(named.astype(BF16), earlier)
    kept = (named > 0.5) & (before < cap)
    rank_ref[...] = jnp.where(kept, before, DROPPED)

    plane = zx[0] * NX
    eight = lax.broadcasted_iota(jnp.int32, (8, toks), 0) + plane
    held_lane = lax.broadcasted_iota(jnp.int32, (8, half), 1)
    held_row = lax.broadcasted_iota(jnp.int32, (8, half), 0) + plane
    room = jnp.sum(jnp.where(held_lane == held_row, home, 0.0), axis=1, keepdims=True)
    room = jnp.where(low, room, float(CAP_OWN))

    pl.semaphore_wait(barrier, last + 3)

    mid = nz // 2

    def meta_copy(n):
        pz = lax.rem(zx[0] + toward(n) + nz, nz)
        return pltpu.make_async_remote_copy(
            src_ref=meta_ref.at[0],
            dst_ref=meta_ref.at[n],
            send_sem=msend.at[n],
            recv_sem=mrecv.at[n],
            device_id={"expert": pz * NX + zx[1]},
            device_id_type=MESH,
        )

    def block_hop(c, t, source=None):
        half_of, back = c % 2, c // 2
        if source is None:
            source = blk_ref.at[2 * t - 3 + back, half_of]
        pz = lax.rem(zx[0] + (nz - 1 if back else 1), nz)
        return pltpu.make_async_remote_copy(
            src_ref=source,
            dst_ref=blk_ref.at[2 * t - t // mid if back else 2 * t - 1, half_of],
            send_sem=gsend.at[c, t],
            recv_sem=grecv.at[c, t],
            device_id={"expert": pz * NX + zx[1]},
            device_id_type=MESH,
        )

    def meta_issue(n, c):
        meta_copy(n).start()
        return c

    for c in (0, 3, 1, 2):
        block_hop(c, 1, (tok_ref, cot_ref)[c % 2]).start()
    lax.fori_loop(1, nz, meta_issue, 0)

    def side_copy(src, dst, send, recv, k):
        peer = plane + lax.rem(zx[1] + lax.rem(k, NX), NX)
        return pltpu.make_async_remote_copy(
            src_ref=src.at[k],
            dst_ref=dst.at[k],
            send_sem=send.at[k],
            recv_sem=recv.at[k],
            device_id={"expert": peer},
            device_id_type=MESH,
        )

    def base_copy(k):
        return side_copy(base_ref, rb_ref, bsend, brecv, k)

    def ext_copy(k):
        return side_copy(ext_ref, re_ref, esend, erecv, k)

    def pack(b, xs, cots):
        ids = meta_ref[b, :top, :]
        share_of = meta_ref[b, top:, :]
        named = jnp.zeros((8, toks), F32)
        weight = jnp.zeros((8, toks), F32)
        for k in range(top):
            hit = ids[k : k + 1, :] == eight.astype(F32)
            named += jnp.where(hit, 1.0, 0.0)
            weight += jnp.where(hit, share_of[k : k + 1, :], 0.0)
        before = dot(named.astype(BF16), earlier)
        seen_ref[...] = jnp.where((named > 0.5) & (before < room), before, DROPPED)
        seen_pw_ref[...] = weight
        shape = (NX, 16, toks)
        slot = lax.broadcasted_iota(jnp.int32, shape, 1).astype(F32)
        ranks = jnp.broadcast_to(seen_ref[:NX, :].reshape(NX, 1, toks), shape)
        weights = jnp.broadcast_to(seen_pw_ref[:NX, :].reshape(NX, 1, toks), shape)
        pick = jnp.where((ranks == slot) & (slot < 7.5), 1.0, 0.0).reshape(NX * 16, toks).astype(BF16)
        scale = jnp.where(ranks == slot - 8.0, weights, 0.0).reshape(NX * 16, toks).astype(BF16)
        rows = (dot(pick, xs[...]) + dot(scale, cots[...])).reshape(NX, 16, d).astype(BF16)
        for r in range(NX):
            base_ref[b * NX + lax.rem(r - zx[1] + NX, NX)] = rows[r]

        @pl.when(low)
        def _():
            shape = (NX, 8, toks)
            place = lax.broadcasted_iota(jnp.int32, shape, 1)
            ranks = jnp.broadcast_to(seen_ref[:NX, :].reshape(NX, 1, toks), shape)
            weights = jnp.broadcast_to(seen_pw_ref[:NX, :].reshape(NX, 1, toks), shape)
            here = ranks == (8 + place % 2).astype(F32)
            total = jnp.zeros((NX * 8, wide), F32)
            for q in range(2):
                pick = jnp.where(here & (place // 2 == 2 * q), 1.0, 0.0).reshape(NX * 8, toks).astype(BF16)
                scale = jnp.where(here & (place // 2 == 2 * q + 1), weights, 0.0).reshape(NX * 8, toks).astype(BF16)
                cols = slice(q * wide, (q + 1) * wide)
                total += dot(pick, xs[:, cols]) + dot(scale, cots[:, cols])
            total = total.reshape(NX, 8, wide).astype(BF16)
            for r in range(NX):
                ext_ref[b * NX + lax.rem(r - zx[1] + NX, NX)] = total[r]
            re_ref[b * NX] = ext_ref[b * NX]

        rb_ref[b * NX] = base_ref[b * NX]
        for j in range(1, NX):
            base_copy(b * NX + j).start()

            @pl.when(low)
            def _():
                ext_copy(b * NX + j).start()

    pack(0, tok_ref, cot_ref)

    for load in loads:
        load.wait()

    many = 16
    rows = many * 10

    def v_copy(k):
        oz, ox = origin(k, nz, zx)
        return pltpu.make_async_remote_copy(
            src_ref=v_ref.at[k],
            dst_ref=vr_ref.at[me],
            send_sem=vsend.at[k],
            recv_sem=vrecv.at[k],
            device_id={"expert": oz * NX + ox},
            device_id_type=MESH,
        )

    def v_issue(k, c):
        @pl.when(k > 0)
        def _():
            v_copy(k).start()

        return c

    def on_group(g, c):
        def arrive(i, c2):
            k = g * many + i

            @pl.when(lax.rem(k, NX) > 0)
            def _():
                base_copy(k).wait_recv()

            @pl.when((lax.rem(k, NX) > 0) & low)
            def _():
                ext_copy(k).wait_recv()

            return c2

        lax.fori_loop(0, many, arrive, 0)
        src = pl.ds(pl.multiple_of(g * many, many), many)
        at = pl.multiple_of(g * rows, 32)
        part = rb_ref[src].astype(F32)
        x_ref[pl.ds(at, many * 8), :] = part[:, :8, :].reshape(many * 8, d).astype(BF16)
        s_ref[pl.ds(at, many * 8), :] = part[:, 8:, :].reshape(many * 8, d).astype(BF16)
        extra = re_ref[src].astype(F32).reshape(many * 8, wide)
        extra = jnp.where(low, extra, 0.0).astype(BF16)
        out_row = lax.broadcasted_iota(jnp.int32, (4 * many, many * 8), 0)
        in_row = lax.broadcasted_iota(jnp.int32, (4 * many, many * 8), 1)
        wanted = (out_row % many) * 8 + out_row // many
        for q in range(2):
            pick = jnp.where(in_row == wanted + 4 * q, 1.0, 0.0).astype(BF16)
            both = dot(pick, extra).astype(BF16)
            cols = slice(q * wide, (q + 1) * wide)
            x_ref[pl.ds(at + many * 8, many * 2), cols] = both[: 2 * many]
            s_ref[pl.ds(at + many * 8, many * 2), cols] = both[2 * many :]
        here = pl.ds(at, rows)
        x, s = x_ref[here, :], s_ref[here, :]
        a = dot(x, wg_ref[...])
        b = dot(x, wu_ref[...])
        sig = jax.nn.sigmoid(a)
        silu = a * sig
        hidden = (silu * b).astype(BF16)
        h_ref[here, :] = hidden
        cot = dot(s, wd_ref[...], ((1,), (1,)))
        pg_ref[here, :] = (cot * b * sig * (1.0 + a * (1.0 - sig))).astype(BF16)
        pu_ref[here, :] = (cot * silu).astype(BF16)
        out = dot(hidden, wd_ref[...])
        col = jnp.sum(out * s.astype(F32), axis=1, keepdims=True)
        own = lax.broadcasted_iota(jnp.int32, (many * 8, 128), 1)
        sub = lax.broadcasted_iota(jnp.int32, (many * 8, 128), 0) % 8
        tile = jnp.sum(jnp.where(own == sub, col[: many * 8], 0.0).reshape(many, 8, 128), axis=1)
        own = lax.broadcasted_iota(jnp.int32, (many, 128), 1)
        for j in range(2):
            tile += jnp.where(own == 8 + j, col[many * (8 + j) : many * (9 + j)], 0.0)
        v_ref[src] = tile.reshape(many, 1, 128)
        return c

    groups = experts // many

    def do_group(g, c):
        on_group(g, c)
        lax.fori_loop(g * many, g * many + many, v_issue, 0)
        return c

    def on_pair(i, b):
        meta_copy(b + i).wait_recv()
        pack(b + i, blk_ref.at[b + i, 0], blk_ref.at[b + i, 1])
        return b

    def on_step(t, c):
        for c4 in (0, 3, 1, 2):
            block_hop(c4, t, tok_ref).wait_recv()
            if c4 in (0, 3):
                block_hop(c4, t + 1).start()
            else:

                @pl.when(t < mid - 1)
                def _():
                    block_hop(c4, t + 1).start()

        lax.fori_loop(0, 2, on_pair, 2 * t - 1)

        @pl.when((t > 2) & (lax.rem(t, 2) == 1))
        def _():
            do_group((t - 3) // 2, 0)

        return c

    lax.fori_loop(1, mid, on_step, 0)
    for c in (0, 3):
        block_hop(c, mid, tok_ref).wait_recv()
    meta_copy(nz - 1).wait_recv()
    pack(nz - 1, blk_ref.at[nz - 1, 0], blk_ref.at[nz - 1, 1])
    on_group(groups - 1, 0)

    far = ny // 2
    parts = (
        (gate_ref, peer_g, out_g, in_g),
        (up_ref, peer_u, out_u, in_u),
        (dl_ref, peer_l, out_l, in_l),
        (dr_ref, peer_r, out_r, in_r),
    )
    ways = (1, -1)

    def length(i, w):
        return far if (i % 2 == 0) == (w == 0) else ny - 1 - far

    def chip(off):
        return lax.rem(y + off + ny, ny)

    def across(i, off):
        src, dst, _, _ = parts[i]
        o = chip(off)
        return pltpu.make_async_remote_copy(
            src_ref=src.at[o, other],
            dst_ref=dst.at[o],
            send_sem=dsend.at[i, off % ny],
            recv_sem=drecv.at[i, off % ny],
            device_id={"dp": y * 2 + other},
            device_id_type=MESH,
        )

    def hop(i, w, t):
        _, _, out, inn = parts[i]
        at = w * far + t
        return pltpu.make_async_remote_copy(
            src_ref=out.at[at],
            dst_ref=inn.at[at],
            send_sem=rsend.at[i, at],
            recv_sem=rrecv.at[i, at],
            device_id={"dp": ahead if w == 0 else behind},
            device_id_type=MESH,
        )

    share, few = gate_ref.shape[2], dl_ref.shape[2]

    def product(off):
        o = chip(off)
        xs = x_ref[:, pl.ds(pl.multiple_of(o * 2 * share, 2 * share), 2 * share)]
        gate_ref[o] = dot(xs, pg_ref[...], turn).reshape(2, share, ff).astype(BF16)
        up_ref[o] = dot(xs, pu_ref[...], turn).reshape(2, share, ff).astype(BF16)

    def cross(off, which):
        for i in which:
            across(i, off).start()

    joined = set()

    def local(i, off):
        if (i, off % ny) not in joined:
            joined.add((i, off % ny))
            across(i, off).wait()
        src, dst, _, _ = parts[i]
        o = chip(off)
        return src[o, core].astype(F32) + dst[o].astype(F32)

    def ring(t):
        chains = [(i, w) for i in range(4) for w in range(2)]
        chains.sort(key=lambda c: -length(*c))
        for i, w in chains:
            if t < length(i, w):
                total = local(i, ways[w] * (length(i, w) - t))
                if t > 0:
                    hop(i, w, t - 1).wait_recv()
                    total = total + parts[i][3][w * far + t - 1].astype(F32)
                parts[i][2][w * far + t] = total.astype(BF16)
                hop(i, w, t).start()

    steps = [far]
    for m in range(far - 1, 0, -1):
        steps += [m, -m]
    steps += [0]
    product(far)
    for ref, at in ((dl_ref, 0), (dr_ref, wide)):
        down = dot(h_ref[...], s_ref[:, at : at + wide], turn)
        ref[...] = down.reshape(ny, 2, few, wide).astype(BF16)
    cross(far, range(4))
    lax.fori_loop(experts - many, experts, v_issue, 0)
    vr_ref[me] = v_ref[0]
    t = 0
    for n, off in enumerate(steps[1:]):
        product(off)
        cross(off, range(4))
        if n % 2 == 1:
            ring(t)
            t += 1
    for rest in range(t, far):
        ring(rest)

    def v_finish(k, c):
        v_copy(k).wait()
        return c

    lax.fori_loop(1, experts, v_finish, 0)
    values = vr_ref[...].reshape(experts, 128)
    place = rank_ref[...]
    back = jnp.zeros((experts, toks), F32)
    for r in range(CAP_OWN + CAP_REP):
        back += jnp.where(place == float(r), values[:, r : r + 1], 0.0)
    for k in range(top):
        mine = jnp.where(ids_ref[k : k + 1, :] == row, back, 0.0)
        gc_out[k : k + 1, :] = jnp.sum(mine, axis=0, keepdims=True) / probs[k : k + 1, :]

    for i, ref in ((0, gate_out), (1, up_out), (2, down_out), (3, down_out)):
        total = local(i, 0)
        for w in range(2):
            if length(i, w) > 0:
                hop(i, w, length(i, w) - 1).wait_recv()
                total = total + parts[i][3][w * far + length(i, w) - 1].astype(F32)
        if i < 2:
            ref[...] = total
        else:
            ref[:, (i - 2) * wide : (i - 1) * wide] = total
    for i in range(4):
        for w in range(2):
            for t in range(length(i, w)):
                hop(i, w, t).wait_send()

    def sent(k, c):
        @pl.when(lax.rem(k, NX) > 0)
        def _():
            base_copy(k).wait_send()

        @pl.when((lax.rem(k, NX) > 0) & low)
        def _():
            ext_copy(k).wait_send()

        return c

    lax.fori_loop(0, experts, sent, 0)

    def told(n, c):
        meta_copy(n).wait_send()
        return c

    lax.fori_loop(1, nz, told, 0)
    for c in range(4):
        for t in range(1, mid + (c in (0, 3))):
            block_hop(c, t, (tok_ref, cot_ref)[c % 2]).wait_send()


def pass_kernel(*refs):
    n = len(refs) // 2
    for src, dst in zip(refs[:n], refs[n:]):
        dst[...] = src[...]


def per_device(tokens, cotangent, expert_ids, gate_probs, home_share, gate_weight, up_weight, down_weight):
    experts = lax.axis_size("expert")
    groups = lax.axis_size("dp")
    nz, ny = experts // NX, groups // 2
    half = experts // 2
    toks, d = tokens.shape
    top = expert_ids.shape[1]
    ff = gate_weight.shape[2]
    wide = d // 2
    share, few = d // groups, ff // groups
    shape = jax.ShapeDtypeStruct
    dma = pltpu.SemaphoreType.DMA
    rows = experts * 10
    gu = (share, ff)
    dn = (few, wide)
    outs = (shape((top, toks), F32), shape(gu, F32), shape(gu, F32), shape((few, d), F32))

    def held(*dims, dtype=BF16):
        return pltpu.VMEM(dims, dtype)

    raw = pl.pallas_call(
        functools.partial(layer_kernel, nz),
        out_shape=outs,
        in_specs=[VMEM] * 5 + [ANY] * 3,
        out_specs=(VMEM,) * 4,
        scratch_shapes=[
            held(experts, toks, dtype=F32),
            held(8, toks, dtype=F32),
            held(8, toks, dtype=F32),
            held(nz, 8, toks, dtype=F32),
            held(nz, 2, toks, d),
            held(experts, 16, d),
            held(experts, 8, wide),
            held(experts, 16, d),
            held(experts, 8, wide),
            held(d, ff),
            held(d, ff),
            held(ff, d),
            held(rows, d),
            held(rows, d),
            held(rows, ff),
            held(rows, ff),
            held(rows, ff),
            held(experts, 1, 128, dtype=F32),
            held(experts, 1, 128, dtype=F32),
        ]
        + [held(ny, 2, *s) for s in (gu, gu, dn, dn)]
        + [held(ny, *s) for s in (gu, gu, dn, dn)]
        + [held(ny, *s) for s in (gu, gu, dn, dn)] * 2
        + [dma((3,))]
        + [dma((experts,))] * 6
        + [dma((nz,))] * 2
        + [dma((4, nz // 2 + 1))] * 2
        + [dma((4, ny))] * 4,
        compiler_params=pltpu.CompilerParams(collective_id=0, has_side_effects=True),
        name="layer",
    )(expert_ids.T, gate_probs.T, home_share[None], tokens, cotangent, gate_weight[0], up_weight[0], down_weight[0])
    gc, gg, gup, gdn = pl.pallas_call(
        pass_kernel, out_shape=outs, in_specs=[VMEM] * 4, out_specs=(VMEM,) * 4, name="hand_on"
    )(*raw)
    return gc.T, gg[None], gup[None], gdn[None]


def solution(mesh):
    rows = P(("dp", "expert"), None)
    held = P("expert", None, None)
    split = P("expert", "dp", None)
    return jax.shard_map(
        per_device,
        mesh=mesh,
        in_specs=(rows, rows, rows, rows, P(), held, held, held),
        out_specs=(rows, split, split, split),
        check_vma=False,
    )
```
